256 devices in a mesh: grp: 2 (over y), mode: 64 (over x, z), node: 2 (over core).
Axes of the slice: x: 4, y: 2, z: 16, core: 2. Of those that a mesh axis runs over, the one named last changes fastest.
The devices are a block of a 4x16x16 slice.
Arguments:
- mode_basis: float32 [4096, 32768], P('mode', 'node'), may hold values from -16 to 16
- mode_scales: float32 [4096], P('mode'), may hold values from 0.003 to 0.02
- mean_log: float32 [32768], P(('node', 'mode')), may hold values from -0.5 to 0.5
- sample_seeds: int32 [4096], P('grp'), parts along dimension 0, may hold values from 0 to 1073741823
Outputs:
- modulus: float32 [32768, 4096], P(('node', 'mode'), 'grp'), parts along dimension 1
- sample_means: float32 [4096], P('grp'), parts along dimension 0
The draws below stay inside these ranges and needn't reach their ends.
There are 2 independent parts, one for each index of `grp`. The reference program is written for one: setup_inputs(seed, part) draws one part's arguments, and reference() takes and returns one part's arrays. A program takes and returns all parts, laid end to end along the dimension named above; an argument that names none is the same for every part. Nothing has to cross between parts.
All inputs are finite; a program needn't handle non-finite values.
Results may differ from the reference program's by a relative error of at most 0.00005.
Values sent between devices are 32-bit elements; how exact they have to be, the bound alone decides.
A program may use at most 64 MiB of HBM per device.

```python
import math
import jax
import jax.numpy as jnp
from jax import lax

MODES = 4096
SAMPLES = 2048
NODES = 32768


def plant(entries, own_key, smallest, top_value):
    spot = [jax.random.randint(jax.random.fold_in(own_key, axis), (), 0, length) for axis, length in enumerate(entries.shape)]
    widest = entries.shape.index(max(entries.shape))
    neighbour = spot[:widest] + [(spot[widest] + 1) % entries.shape[widest]] + spot[widest + 1:]
    return entries.at[tuple(spot)].set(smallest).at[tuple(neighbour)].set(top_value)


def with_spikes(array, own_key, source, target, blocks, factor):
    owner, partner = [(jnp.arange(array.shape[axis_at]) // (array.shape[axis_at] // blocks)).reshape([-1 if axis == axis_at else 1 for axis in range(array.ndim)]) for axis_at in (source, target)]
    chosen = jax.random.permutation(own_key, blocks)[partner]
    strong = (owner == chosen) | (owner == (partner + blocks // 2) % blocks)
    return jnp.where(strong, factor * array, array)


def level_of(stream_key, dims, split, low, high):
    loudness, own = 1.0, jax.random.fold_in(stream_key, 6)
    for axis_at, shards_of in split:
        draws = jnp.exp(jax.random.uniform(jax.random.fold_in(own, axis_at), (shards_of,), jnp.float32, low / len(split), high / len(split)))
        loudness = loudness * jnp.repeat(draws, dims[axis_at] // shards_of).reshape([-1 if axis == axis_at else 1 for axis in range(len(dims))])
    return loudness


def bell_draw_with(rng, shape, spread, reach, pieces, heavy, kind=jnp.bfloat16):
    entries = spread * jax.random.normal(rng, shape, jnp.float32)
    if pieces:
        entries = entries * level_of(rng, shape, pieces, -0.22, 0.18)
    return jnp.clip(with_spikes(entries, jax.random.fold_in(rng, 3), *heavy), -reach, reach).astype(kind)


def setup_inputs(seed: int = 0, part: int = 0) -> dict:
    key_of = jax.random.split(jax.random.key(seed), 5)
    own_keys = jax.random.split(jax.random.fold_in(key_of[4], part), 5)
    return {
        "mode_basis": bell_draw_with(key_of[0], (MODES, NODES), 1.0, 16.0, ((0, 64), (1, 2)), (0, 1, 64, 4.0), jnp.float32),
        "mode_scales": jnp.clip(jnp.exp(math.log(0.02) - 1.89712 * jax.random.uniform(key_of[1], (MODES,), jnp.float32) ** level_of(key_of[1], (MODES,), ((0, 64),), -0.2, 0.2)), 0.003, 0.02),
        "mean_log": jnp.clip(jax.random.uniform(key_of[2], (NODES,), jnp.float32, -0.5, 0.5) * level_of(key_of[2], (NODES,), ((0, 128),), -0.4, 0.0), -0.5, 0.5),
        "sample_seeds": plant(jax.random.randint(own_keys[3], (SAMPLES,), 0, 1073741824), jax.random.fold_in(own_keys[3], 1), 0, 1073741823).astype(jnp.int32),
    }


def scramble(seed_words, counter_words):
    mixed_word = seed_words * -1640531527 + counter_words * 668265261
    mixed_word = mixed_word ^ mixed_word >> 15 & 131071
    mixed_word = mixed_word * -2048144789
    mixed_word = mixed_word ^ mixed_word >> 13 & 524287
    mixed_word = mixed_word * -1028477387
    mixed_word = mixed_word ^ mixed_word >> 16 & 65535
    return mixed_word

def normals(sample_seeds, mode_start, mode_count):
    mode_ids = mode_start + jnp.arange(mode_count, dtype=jnp.int32)
    seed_words = sample_seeds.astype(jnp.int32)[None, :]
    counter_words = (2 * mode_ids).astype(jnp.int32)[:, None]
    first_word = scramble(seed_words, counter_words)
    second_word = scramble(seed_words, counter_words + 1)
    first_unit = ((first_word & 16777215).astype(jnp.float32) + 0.5) * (1.0 / 16777216.0)
    second_unit = ((second_word & 16777215).astype(jnp.float32) + 0.5) * (1.0 / 16777216.0)
    radius = jnp.sqrt(-2.0 * jnp.log(first_unit))
    return radius * jnp.cos(2.0 * math.pi * second_unit)

def reference(mode_basis, mode_scales, mean_log, sample_seeds):
    scaled = mode_scales[:, None] * mode_basis
    coeffs = normals(sample_seeds, 0, MODES)
    summed = lax.dot_general(scaled, coeffs, (((0,), (0,)), ((), ())), precision=lax.Precision.HIGHEST, preferred_element_type=jnp.float32)
    modulus = jnp.exp(mean_log[:, None] + summed)
    sample_means = lax.optimization_barrier(jnp.sum(modulus, axis=0)) / NODES
    return (modulus, sample_means)
```

```python
import functools
import math

import jax
import jax.numpy as jnp
from jax import lax
from jax.experimental import pallas as pl
from jax.experimental.pallas import tpu as pltpu
from jax.sharding import PartitionSpec as P

MESH = pl.DeviceIdType.MESH
X, Z = 4, 16
C1, C2 = -1640531527, 668265261
H1, H2 = -2048144789, -1028477387
CHUNK = 256
GEN_ROWS, GEN_COLS = 16, 512


def wrap32(value):
    return ((value + 2**31) % 2**32) - 2**31


SINE_TURNS = (6.283185160089197, -41.3416550313564, 81.60100406980851, -76.54978221989163, 39.536705541154184)
SINE = [c * math.sqrt(2.0) for c in SINE_TURNS]


def mix(word):
    word = word ^ lax.shift_right_logical(word, 15)
    word = word * H1
    word = word ^ lax.shift_right_logical(word, 13)
    word = word * H2
    return word ^ lax.shift_right_logical(word, 16)


def normals_tile(seed_part, mode_part):
    start = seed_part + mode_part
    first = mix(start)
    second = mix(start + C2)
    unit = ((first & 16777215).astype(jnp.float32) + 0.5) * (1.0 / 16777216.0)
    minus_log = jnp.maximum(-jnp.log(unit), 1e-30)
    radius = minus_log * lax.rsqrt(minus_log)
    turn = (lax.shift_left(second, 8) | 128).astype(jnp.float32)
    w = 0.25 - jnp.abs(turn * (1.0 / 4294967296.0))
    s = w * w
    p = SINE[4]
    for c in (SINE[3], SINE[2], SINE[1], SINE[0]):
        p = p * s + c
    return radius * (p * w)


def kernel(
    groups, basis, scales, mean_log, seeds, out_hbm, means_out,
    send_buf, recv, chi, clo, acc, seed_rows, mode_col, part, bufa, s1, bufb, s2, bufc, fin,
    load_sem, tx_sem, rx_sem, ytx_sem, yrx_sem, red_tx, red_rx, out_sem,
):
    own = X * Z // groups
    per_chunk = CHUNK // 64
    own_chunks = own // per_chunk
    right_hops, left_hops = groups // 2, (groups - 1) // 2
    samples = seeds.shape[1]
    half = samples // 2

    grp = lax.axis_index("grp")
    me = lax.axis_index("mode")
    core = lax.axis_index("node")
    x, z = me // Z, lax.rem(me, Z)

    def displacement(plane, i):
        e = i * groups + plane
        zi = e // X
        k = (zi + 1) // 2
        dz = jnp.where(lax.rem(zi, 2) == 1, k, Z - k)
        return e, lax.rem(e, X), lax.rem(dz, Z)

    def peer(dx, dz, sign):
        px = lax.rem(x + sign * dx + X, X)
        pz = lax.rem(z + sign * dz + Z, Z)
        return px * Z + pz

    right = lax.rem(grp + 1, groups)
    left = lax.rem(grp + groups - 1, groups)

    def load(i):
        _, dx, dz = displacement(grp, i)
        col = pl.multiple_of(peer(dx, dz, 1) * 256, 256)
        return pltpu.make_async_copy(basis.at[:, pl.ds(col, 256)], send_buf.at[i], load_sem.at[i])

    @pl.loop(0, own)
    def _(i):
        load(i).start()

    bar = pltpu.get_barrier_semaphore()

    def hello(**where):
        pl.semaphore_signal(bar, 1, device_id=where, device_id_type=MESH)

    @pl.loop(0, own)
    def _(i):
        e, dx, dz = displacement(grp, i)

        @pl.when(e != 0)
        def _():
            hello(mode=peer(dx, dz, -1))

    @pl.loop(1, Z)
    def _(k):
        hello(mode=peer(0, k, 1))

    @pl.loop(1, X)
    def _(k):
        hello(mode=peer(k, 0, 1))

    hello(node=1 - core)
    if right_hops:
        hello(grp=left)
    if left_hops:
        hello(grp=right)

    row64 = lax.broadcasted_iota(jnp.int32, (64, 64), 0)
    col64 = lax.broadcasted_iota(jnp.int32, (64, 64), 1)
    scale_col = jnp.sum(
        jnp.where(row64 == col64, jnp.broadcast_to(scales[...], (64, 64)), 0.0), axis=1, keepdims=True
    )
    mode_col[...] = jnp.broadcast_to(scale_col, mode_col.shape)

    @pl.loop(0, own)
    def _(i):
        load(i).wait()
        send_buf[i] = send_buf[i] * mode_col[...]

    expected = jnp.where(grp == 0, own - 1, own) + (Z - 1) + (X - 1) + 1
    expected = expected + (1 if right_hops else 0) + (1 if left_hops else 0)
    pl.semaphore_wait(bar, expected)

    def piece(i):
        _, dx, dz = displacement(grp, i)
        return pltpu.make_async_remote_copy(
            src_ref=send_buf.at[i],
            dst_ref=recv.at[pl.ds(pl.multiple_of(i * 64, 64), 64), :],
            send_sem=tx_sem.at[i],
            recv_sem=rx_sem.at[i],
            device_id={"mode": peer(dx, dz, 1)},
            device_id_type=MESH,
        )

    @pl.loop(0, own)
    def _(i):
        e, _, _ = displacement(grp, i)

        @pl.when(e != 0)
        def _():
            piece(i).start()

        @pl.when(e == 0)
        def _():
            recv[0:64, :] = send_buf[0]

    def hop(source_block, target_block, i, to):
        src = pl.multiple_of((source_block * own + i) * 64, 64)
        dst = pl.multiple_of((target_block * own + i) * 64, 64)
        slot = (target_block - 1) * own + i
        return pltpu.make_async_remote_copy(
            src_ref=recv.at[pl.ds(src, 64), :],
            dst_ref=recv.at[pl.ds(dst, 64), :],
            send_sem=ytx_sem.at[slot],
            recv_sem=yrx_sem.at[slot],
            device_id={"grp": to},
            device_id_type=MESH,
        )

    nodes = acc.shape[0]
    row_n = lax.broadcasted_iota(jnp.int32, (nodes, nodes), 0)
    col_n = lax.broadcasted_iota(jnp.int32, (nodes, nodes), 1)
    mean_col = jnp.sum(
        jnp.where(row_n == col_n, jnp.broadcast_to(mean_log[...], (nodes, nodes)), 0.0), axis=1, keepdims=True
    )
    acc[...] = jnp.broadcast_to(mean_col, acc.shape)
    seed_rows[...] = jnp.broadcast_to(seeds[...] * C1, seed_rows.shape)

    row_ids = lax.broadcasted_iota(jnp.int32, (GEN_ROWS, GEN_COLS), 0) * wrap32(2 * C2)

    def generate(block, plane, chunk):
        @pl.loop(0, CHUNK // GEN_ROWS)
        def _(r):
            i = chunk * per_chunk + r // (64 // GEN_ROWS)
            _, dx, dz = displacement(plane, i)
            first_mode = peer(dx, dz, -1) * 64 + lax.rem(r, 64 // GEN_ROWS) * GEN_ROWS
            mode_part = row_ids + first_mode * wrap32(2 * C2)
            rows = pl.ds(pl.multiple_of(block * own * 64 + chunk * CHUNK + r * GEN_ROWS, GEN_ROWS), GEN_ROWS)
            for c in range(samples // GEN_COLS):
                cols = slice(c * GEN_COLS, (c + 1) * GEN_COLS)
                value = normals_tile(seed_rows[:, cols], mode_part)
                high = value.astype(jnp.bfloat16)
                chi[rows, cols] = high
                clo[rows, cols] = (value - high.astype(jnp.float32)).astype(jnp.bfloat16)

    def contract(block, chunk):
        rows = pl.ds(pl.multiple_of(block * own * 64 + chunk * CHUNK, CHUNK), CHUNK)
        lhs = recv[rows, :].T
        high = lhs.astype(jnp.bfloat16)
        low = (lhs - high.astype(jnp.float32)).astype(jnp.bfloat16)
        dot = functools.partial(jnp.dot, preferred_element_type=jnp.float32)
        for c in range(samples // 256):
            cols = slice(c * 256, (c + 1) * 256)
            c_high = chi[rows, cols]
            acc[:, cols] += dot(high, c_high) + dot(low, c_high) + dot(high, clo[rows, cols])

    def ring_block(b):
        hops = (b + 1) // 2
        to_right = lax.rem(b, 2) == 1
        plane = lax.rem(jnp.where(to_right, grp - hops, grp + hops) + groups, groups)
        return hops, to_right, plane

    def ring_forward(b, i):
        hops, to_right, _ = ring_block(b)

        @pl.when(jnp.logical_and(to_right, hops < right_hops))
        def _():
            hop(b, b + 2, i, right).start()

        @pl.when(jnp.logical_and(jnp.logical_not(to_right), hops < left_hops))
        def _():
            hop(b, b + 2, i, left).start()

    @pl.loop(0, own_chunks + 1)
    def _(j):
        @pl.when(j < own_chunks)
        def _():
            generate(0, grp, j)
            if groups > 1:
                generate(1, ring_block(1)[2], j)

            @pl.loop(0, per_chunk)
            def _(p):
                i = j * per_chunk + p
                e, _, _ = displacement(grp, i)

                @pl.when(e != 0)
                def _():
                    piece(i).wait()

                if right_hops:
                    hop(0, 1, i, right).start()
                if left_hops:
                    hop(0, 2, i, left).start()

            contract(0, j)

        if groups > 1:

            @pl.when(j > 0)
            def _():
                @pl.loop(1, groups)
                def _(b):
                    _, _, plane = ring_block(b)

                    @pl.when(b > 1)
                    def _():
                        generate(b, plane, j - 1)

                    @pl.loop(0, per_chunk)
                    def _(p):
                        i = (j - 1) * per_chunk + p
                        hop(b, b, i, right).wait()
                        ring_forward(b, i)

                    contract(b, j - 1)

    for c in range(samples // 256):
        cols = slice(c * 256, (c + 1) * 256)
        value = jnp.exp(acc[:, cols])
        acc[:, cols] = value
        part[:, cols] = jnp.sum(value, axis=0, keepdims=True)
    store = pltpu.make_async_copy(acc, out_hbm, out_sem)
    store.start()

    mine = pl.ds(pl.multiple_of(core * half, 128), half)
    other = pl.ds(pl.multiple_of((1 - core) * half, 128), half)
    swap = pltpu.make_async_remote_copy(
        src_ref=part.at[:, other], dst_ref=bufa, send_sem=red_tx.at[0], recv_sem=red_rx.at[0],
        device_id={"node": 1 - core}, device_id_type=MESH,
    )
    swap.start()
    swap.wait()
    s1[...] = part[:, mine] + bufa[...]

    def along(buffer, source, k, dx, dz, slot, row):
        return pltpu.make_async_remote_copy(
            src_ref=source, dst_ref=buffer.at[row], send_sem=red_tx.at[slot], recv_sem=red_rx.at[slot],
            device_id={"mode": peer(dx, dz, 1)}, device_id_type=MESH,
        )

    @pl.loop(1, X)
    def _(k):
        along(bufb, s1, k, k, 0, k, x).start()

    bufb[x] = s1[...]

    @pl.loop(1, X)
    def _(k):
        along(bufb, s1, k, k, 0, k, lax.rem(x + X - k, X)).wait()

    s2[...] = (bufb[0] + bufb[1]) + (bufb[2] + bufb[3])

    @pl.loop(1, Z)
    def _(k):
        along(bufc, s2, k, 0, k, X + k, z).start()

    bufc[z] = s2[...]

    @pl.loop(1, Z)
    def _(k):
        along(bufc, s2, k, 0, k, X + k, lax.rem(z + Z - k, Z)).wait()

    total = bufc[0]
    for k in range(1, Z):
        total = total + bufc[k]
    node_count = nodes * X * Z * 2
    fin[...] = total * (1.0 / node_count)
    back = pltpu.make_async_remote_copy(
        src_ref=fin, dst_ref=means_out.at[:, mine], send_sem=red_tx.at[X + Z], recv_sem=red_rx.at[X + Z],
        device_id={"node": 1 - core}, device_id_type=MESH,
    )
    back.start()
    means_out[:, mine] = fin[...]
    back.wait_send()
    pltpu.make_async_remote_copy(
        src_ref=fin, dst_ref=means_out.at[:, other], send_sem=red_tx.at[X + Z], recv_sem=red_rx.at[X + Z],
        device_id={"node": 1 - core}, device_id_type=MESH,
    ).wait_recv()
    store.wait()


def solution(mesh):
    groups = mesh.shape["grp"]

    def on_device(mode_basis, mode_scales, mean_log, sample_seeds):
        modes = mode_basis.shape[0]
        nodes, samples = mean_log.shape[0], sample_seeds.shape[0]
        all_modes = modes * X * Z
        own = X * Z // groups
        half = samples // 2
        f32 = jnp.float32
        vmem = pl.BlockSpec(memory_space=pltpu.VMEM)
        modulus, means = pl.pallas_call(
            functools.partial(kernel, groups),
            out_shape=(jax.ShapeDtypeStruct((nodes, samples), f32), jax.ShapeDtypeStruct((1, samples), f32)),
            in_specs=[pl.BlockSpec(memory_space=pl.ANY), vmem, vmem, vmem],
            out_specs=(pl.BlockSpec(memory_space=pl.ANY), vmem),
            scratch_shapes=[
                pltpu.VMEM((own, modes, nodes), f32),
                pltpu.VMEM((all_modes, nodes), f32),
                pltpu.VMEM((all_modes, samples), jnp.bfloat16),
                pltpu.VMEM((all_modes, samples), jnp.bfloat16),
                pltpu.VMEM((nodes, samples), f32),
                pltpu.VMEM((GEN_ROWS, samples), jnp.int32),
                pltpu.VMEM((modes, nodes), f32),
                pltpu.VMEM((1, samples), f32),
                pltpu.VMEM((1, half), f32),
                pltpu.VMEM((1, half), f32),
                pltpu.VMEM((X, 1, half), f32),
                pltpu.VMEM((1, half), f32),
                pltpu.VMEM((Z, 1, half), f32),
                pltpu.VMEM((1, half), f32),
                pltpu.SemaphoreType.DMA((own,)),
                pltpu.SemaphoreType.DMA((own,)),
                pltpu.SemaphoreType.DMA((own,)),
                pltpu.SemaphoreType.DMA((max(groups - 1, 1) * own,)),
                pltpu.SemaphoreType.DMA((max(groups - 1, 1) * own,)),
                pltpu.SemaphoreType.DMA((X + Z + 1,)),
                pltpu.SemaphoreType.DMA((X + Z + 1,)),
                pltpu.SemaphoreType.DMA,
            ],
            compiler_params=pltpu.CompilerParams(
                collective_id=0, has_side_effects=True, vmem_limit_bytes=60 * 1024 * 1024
            ),
        )(mode_basis, mode_scales[None, :], mean_log[None, :], sample_seeds[None, :])
        return modulus, means[0]

    return jax.shard_map(
        on_device,
        mesh=mesh,
        in_specs=(P("mode", "node"), P("mode"), P(("node", "mode")), P("grp")),
        out_specs=(P(("node", "mode"), "grp"), P("grp")),
        check_vma=False,
    )
```

```python
import functools
import math

import jax
import jax.numpy as jnp
from jax import lax
from jax.experimental import pallas as pl
from jax.experimental.pallas import tpu as pltpu
from jax.sharding import PartitionSpec as P

MESH = pl.DeviceIdType.MESH
X, Z = 4, 16
C1, C2 = -1640531527, 668265261
H1, H2 = -2048144789, -1028477387
OFFSETS = (8, 7, -7, 4, -4, 6, -6, 3, -3, 5, -5, 2, -2, 1, -1, 0)
SPLIT = 13
AHEAD = 3
LEAD = 9
GEN_ROWS, GEN_COLS = 16, 512


def pieces_sent(groups):
    if groups > X:
        return X * Z // groups
    return SPLIT * (X // groups) + (Z - SPLIT) * X


def wrap32(value):
    return ((value + 2**31) % 2**32) - 2**31


SINE_TURNS = (6.283185160089197, -41.3416550313564, 81.60100406980851, -76.54978221989163, 39.536705541154184)
SINE = [c * math.sqrt(2.0) for c in SINE_TURNS]


def mix(word):
    word = word ^ lax.shift_right_logical(word, 15)
    word = word * H1
    word = word ^ lax.shift_right_logical(word, 13)
    word = word * H2
    return word ^ lax.shift_right_logical(word, 16)


def normals_tile(seed_part, mode_part):
    start = seed_part + mode_part
    first = mix(start)
    second = mix(start + C2)
    unit = ((first & 16777215).astype(jnp.float32) + 0.5) * (1.0 / 16777216.0)
    minus_log = jnp.maximum(-jnp.log(unit), 1e-30)
    radius = minus_log * lax.rsqrt(minus_log)
    turn = (lax.shift_left(second, 8) | 128).astype(jnp.float32)
    w = 0.25 - jnp.abs(turn * (1.0 / 4294967296.0))
    s = w * w
    p = SINE[4]
    for c in (SINE[3], SINE[2], SINE[1], SINE[0]):
        p = p * s + c
    return radius * (p * w)


def kernel(
    groups, basis, scales, mean_log, seeds, out_hbm, means_out,
    small_s, small_m, small_d, send_buf, recv, chi, clo, acc, seed_rows, mode_col, part, row_buf, row_sum, col_buf, fin,
    in_sem, load_sem, tx_sem, rx_sem, ytx_sem, yrx_sem, red_tx, red_rx, out_sem,
):
    own = pieces_sent(groups)
    rows = basis.shape[0]
    chunk_rows = X * rows
    per = max(X // groups, 1)
    right_hops, left_hops = groups // 2, (groups - 1) // 2
    samples = seeds.shape[1]
    cores = lax.axis_size("node")
    nodes = acc.shape[0]

    grp = lax.axis_index("grp")
    me = lax.axis_index("mode")
    core = lax.axis_index("node")
    x, z = me // Z, lax.rem(me, Z)

    def wrap(value, size):
        return jnp.where(value >= size, value - size, value)

    def z_offset(t):
        if isinstance(t, int):
            return OFFSETS[t] % Z
        value = jnp.int32(OFFSETS[-1] % Z)
        for place, offset in enumerate(OFFSETS[:-1]):
            value = jnp.where(t == place, offset % Z, value)
        return value

    def number(plane, i):
        return i * groups + plane

    def ahead(dx, dz):
        return wrap(x + dx, X) * Z + wrap(z + dz, Z)

    def behind(dx, dz):
        return wrap(x - dx + X, X) * Z + wrap(z - dz + Z, Z)

    self_number = OFFSETS.index(0) * X

    def pieces_at(t):
        if t < SPLIT:
            return [(t * per + r, r * groups + grp) for r in range(per)]
        return [(SPLIT * per + (t - SPLIT) * X + dx, dx) for dx in range(X)]

    if groups <= X:
        pieces = [(i, t, dx) for t in range(len(OFFSETS)) for i, dx in pieces_at(t)]
        self_piece = SPLIT * per + (OFFSETS.index(0) - SPLIT) * X
    else:
        pieces = []
        for i in range(own):
            e = number(grp, i)
            pieces.append((i, lax.div(e, X), lax.rem(e, X)))
        self_piece = self_number // groups

    right = lax.rem(grp + 1, groups)
    left = lax.rem(grp + groups - 1, groups)

    bar = pltpu.get_barrier_semaphore()

    def hello(**where):
        pl.semaphore_signal(bar, 1, device_id=where, device_id_type=MESH)

    def row_peer(d):
        q = wrap(x * cores + core + d, X * cores)
        qx = lax.div(q, cores)
        return {"mode": qx * Z + z, "node": q - qx * cores}

    def load(i, t, dx):
        col = pl.multiple_of(ahead(dx, z_offset(t)) * nodes, nodes)
        return pltpu.make_async_copy(basis.at[:, pl.ds(col, nodes)], send_buf.at[i], load_sem.at[i])

    for args in pieces[: AHEAD + 1]:
        load(*args).start()

    columns = [r * groups + grp for r in range(per)] if groups <= X else range(X)

    @pl.loop(0, Z)
    def _(k):
        dz = wrap(k + Z // 2, Z)
        for dx in columns:

            @pl.when(jnp.logical_or(dz != 0, dx != 0))
            def _():
                hello(mode=behind(dx, dz))

        @pl.when(dz != 0)
        def _():
            hello(mode=behind(0, dz))

    beside = [(dx, dz) for dz in (1, Z - 1) for dx in range(1, X)] if groups <= X else []
    for dx, dz in beside:
        hello(mode=behind(dx, dz))

    small = [
        pltpu.make_async_copy(source, target, in_sem.at[k])
        for k, (source, target) in enumerate(((scales, small_s), (mean_log, small_m), (seeds, small_d)))
    ]
    for copy in small:
        copy.start()

    for args in pieces[AHEAD + 1 :]:
        load(*args).start()

    @pl.loop(1, X * cores)
    def _(d):
        hello(**row_peer(d))

    if right_hops:
        hello(grp=left)
    if left_hops:
        hello(grp=right)

    for copy in small:
        copy.wait()
    row64 = lax.broadcasted_iota(jnp.int32, (64, 64), 0)
    col64 = lax.broadcasted_iota(jnp.int32, (64, 64), 1)
    scale_col = jnp.sum(
        jnp.where(row64 == col64, jnp.broadcast_to(small_s[...], (64, 64)), 0.0), axis=1, keepdims=True
    )
    mode_col[...] = jnp.broadcast_to(scale_col, mode_col.shape)

    def scale(i):
        load(i, 0, 0).wait()
        send_buf[i] = send_buf[i] * mode_col[...]

    for i in range(min(AHEAD, own)):
        scale(i)

    own_columns = len(columns) if groups <= X else X
    no_self = jnp.where(grp == 0, 1, 0) if groups <= X else 1
    expected = Z * own_columns - no_self + (Z - 1) + len(beside) + (X * cores - 1)
    expected = expected + (1 if right_hops else 0) + (1 if left_hops else 0)
    pl.semaphore_wait(bar, expected)

    def slot(e):
        return recv.at[pl.ds(pl.multiple_of(e * rows, rows), rows), :]

    def piece(i, t, dx):
        return pltpu.make_async_remote_copy(
            src_ref=send_buf.at[i],
            dst_ref=slot(t * X + dx),
            send_sem=tx_sem.at[i],
            recv_sem=rx_sem.at[i],
            device_id={"mode": ahead(dx, z_offset(t))},
            device_id_type=MESH,
        )

    def send_piece(i, t, dx):
        @pl.when(t * X + dx != self_number)
        def _():
            piece(i, t, dx).start()

    for i, t, dx in pieces:
        if i + AHEAD < own:
            scale(i + AHEAD)
        send_piece(i, t, dx)

    has_self = True if groups <= X else grp == self_number % groups

    @pl.when(has_self)
    def _():
        recv[self_number * rows : (self_number + 1) * rows, :] = send_buf[self_piece]

    def hop(e, direction):
        return pltpu.make_async_remote_copy(
            src_ref=slot(e),
            dst_ref=slot(e),
            send_sem=ytx_sem.at[direction * X * Z + e],
            recv_sem=yrx_sem.at[e],
            device_id={"grp": (right, left)[direction]},
            device_id_type=MESH,
        )

    row_n = lax.broadcasted_iota(jnp.int32, (nodes, nodes), 0)
    col_n = lax.broadcasted_iota(jnp.int32, (nodes, nodes), 1)
    mean_col = jnp.sum(
        jnp.where(row_n == col_n, jnp.broadcast_to(small_m[...], (nodes, nodes)), 0.0), axis=1, keepdims=True
    )
    acc[...] = jnp.broadcast_to(mean_col, acc.shape)
    seed_rows[...] = jnp.broadcast_to(small_d[...] * C1, seed_rows.shape)

    row_ids = lax.broadcasted_iota(jnp.int32, (GEN_ROWS, GEN_COLS), 0) * wrap32(2 * C2)

    def generate(chunk):
        @pl.loop(0, X)
        def _(dx):
            first_mode = behind(dx, z_offset(chunk)) * rows
            first_row = (chunk * X + dx) * rows

            @pl.loop(0, rows // GEN_ROWS)
            def _(r):
                mode_part = row_ids + (first_mode + r * GEN_ROWS) * wrap32(2 * C2)
                at = pl.ds(pl.multiple_of(first_row + r * GEN_ROWS, GEN_ROWS), GEN_ROWS)
                for c in range(samples // GEN_COLS):
                    cols = slice(c * GEN_COLS, (c + 1) * GEN_COLS)
                    value = normals_tile(seed_rows[:, cols], mode_part)
                    high = value.astype(jnp.bfloat16)
                    chi[at, cols] = high
                    clo[at, cols] = (value - high.astype(jnp.float32)).astype(jnp.bfloat16)

    def contract(chunk):
        at = pl.ds(pl.multiple_of(chunk * chunk_rows, chunk_rows), chunk_rows)
        lhs = recv[at, :].T
        high = lhs.astype(jnp.bfloat16)
        low = (lhs - high.astype(jnp.float32)).astype(jnp.bfloat16)
        dot = functools.partial(jnp.dot, preferred_element_type=jnp.float32)
        for c in range(samples // 256):
            cols = slice(c * 256, (c + 1) * 256)
            c_high = chi[at, cols]
            acc[:, cols] += dot(high, c_high) + dot(low, c_high) + dot(high, clo[at, cols])

    def arrive(i, t, dx, travels=True):
        @pl.when(t * X + dx != self_number)
        def _():
            piece(i, t, dx).wait_recv()

        if travels and right_hops:
            hop(t * X + dx, 0).start()
        if travels and left_hops:
            hop(t * X + dx, 1).start()

    def ring_plane(b):
        hops = (b + 1) // 2
        return lax.rem(grp + (groups - hops if b % 2 else hops), groups)

    def goes_on(b):
        return (b + 1) // 2 < (right_hops if b % 2 else left_hops)

    chunks = len(OFFSETS)
    if groups <= X:

        @pl.loop(0, LEAD)
        def _(t):
            generate(t)

        @pl.loop(0, SPLIT + 1)
        def _(t):
            @pl.when(t < SPLIT)
            def _():
                for r in range(per):
                    arrive(t * per + r, t, r * groups + grp)

            @pl.when(t > 0)
            def _():
                for b in range(1, groups):
                    for r in range(per):
                        e = (t - 1) * X + r * groups + ring_plane(b)
                        hop(e, 0).wait_recv()
                        if goes_on(b):
                            hop(e, (b + 1) % 2).start()
                contract(t - 1)

            @pl.when(t + LEAD < chunks)
            def _():
                generate(t + LEAD)

        @pl.loop(SPLIT, chunks)
        def _(t):
            for dx in range(X):
                arrive(SPLIT * per + (t - SPLIT) * X + dx, t, dx, travels=False)
            contract(t)

    else:
        step = chunks // groups

        def generate_some(b):
            @pl.loop(0, step)
            def _(k):
                generate(b * step + k)

        generate_some(0)

        @pl.loop(0, own)
        def _(i):
            e = number(grp, i)
            t = lax.div(e, X)
            arrive(i, t, e - t * X)

        for b in range(1, groups):
            generate_some(b)

            @pl.loop(0, own)
            def _(i, b=b):
                e = number(ring_plane(b), i)
                hop(e, 0).wait_recv()
                if goes_on(b):
                    hop(e, (b + 1) % 2).start()

        @pl.loop(0, chunks)
        def _(t):
            contract(t)

    def all_sent():
        @pl.loop(0, own)
        def _(i):
            @pl.when(jnp.logical_not(jnp.logical_and(has_self, i == self_piece)))
            def _():
                piece(i, 0, 0).wait_send()

        @pl.loop(0, SPLIT * per if groups <= X else own)
        def _(i):
            e = number(grp, i)
            for direction, hops in enumerate((right_hops, left_hops)):
                if hops:
                    hop(e, direction).wait_send()
            for b in range(1, groups):
                if goes_on(b):
                    hop(number(ring_plane(b), i), (b + 1) % 2).wait_send()

    for c in range(samples // 256):
        cols = slice(c * 256, (c + 1) * 256)
        value = jnp.exp(acc[:, cols])
        acc[:, cols] = value
        part[c] = jnp.sum(value, axis=0, keepdims=True)
    store = pltpu.make_async_copy(acc, out_hbm, out_sem)
    store.start()

    me_row = x * cores + core
    width = X * cores

    def row_copy(source, target, d, slot):
        return pltpu.make_async_remote_copy(
            src_ref=source, dst_ref=target, send_sem=red_tx.at[slot], recv_sem=red_rx.at[slot],
            device_id=row_peer(d), device_id_type=MESH,
        )

    @pl.loop(1, width)
    def _(d):
        row_copy(part.at[wrap(me_row + d, width)], row_buf.at[me_row], d, d).start()

    row_buf[me_row] = part[me_row]

    @pl.loop(1, width)
    def _(d):
        row_copy(part.at[me_row], row_buf.at[me_row], d, d).wait()

    total = row_buf[0]
    for k in range(1, width):
        total = total + row_buf[k]
    row_sum[...] = total

    def column_copy(k):
        return pltpu.make_async_remote_copy(
            src_ref=row_sum, dst_ref=col_buf.at[z], send_sem=red_tx.at[width + k], recv_sem=red_rx.at[width + k],
            device_id={"mode": ahead(0, k)}, device_id_type=MESH,
        )

    for k in sorted(range(1, Z), key=lambda k: -min(k, Z - k)):
        column_copy(k).start()

    col_buf[z] = total

    @pl.loop(1, Z)
    def _(k):
        column_copy(k).wait()

    total = col_buf[0]
    for k in range(1, Z):
        total = total + col_buf[k]
    node_count = nodes * X * Z * cores
    fin[...] = total * (1.0 / node_count)

    @pl.loop(1, width)
    def _(d):
        row_copy(fin, means_out.at[me_row], d, width + Z + d).start()

    means_out[me_row] = fin[...]

    @pl.loop(1, width)
    def _(d):
        row_copy(fin, means_out.at[me_row], d, width + Z + d).wait()

    all_sent()
    store.wait()


def hand_over(modulus, means, modulus_out, means_out, held, held_means, in_sem, out_sem):
    parts = in_sem.shape[0] - 1
    rows = modulus.shape[0] // parts
    spans = [pl.ds(k * rows, rows) for k in range(parts)]
    steps = [(modulus.at[at], held.at[at], modulus_out.at[at]) for at in spans] + [(means, held_means, means_out)]
    copies_in = [pltpu.make_async_copy(a, b, in_sem.at[k]) for k, (a, b, _) in enumerate(steps)]
    copies_out = [pltpu.make_async_copy(b, c, out_sem.at[k]) for k, (_, b, c) in enumerate(steps)]
    for copy in copies_in:
        copy.start()
    for arrived, onward in zip(copies_in, copies_out):
        arrived.wait()
        onward.start()
    for copy in copies_out:
        copy.wait()


def solution(mesh):
    groups = mesh.shape["grp"]

    def on_device(mode_basis, mode_scales, mean_log, sample_seeds):
        modes = mode_basis.shape[0]
        nodes, samples = mean_log.shape[0], sample_seeds.shape[0]
        all_modes = modes * X * Z
        own = pieces_sent(groups)
        width = X * mesh.shape["node"]
        share = samples // width
        f32 = jnp.float32
        vmem = pl.BlockSpec(memory_space=pltpu.VMEM)
        modulus, means = pl.pallas_call(
            functools.partial(kernel, groups),
            out_shape=(jax.ShapeDtypeStruct((nodes, samples), f32), jax.ShapeDtypeStruct((width, 1, share), f32)),
            in_specs=[pl.BlockSpec(memory_space=pl.ANY)] * 4,
            out_specs=(pl.BlockSpec(memory_space=pl.ANY), vmem),
            scratch_shapes=[
                pltpu.VMEM((1, modes), f32),
                pltpu.VMEM((1, nodes), f32),
                pltpu.VMEM((1, samples), jnp.int32),
                pltpu.VMEM((own, modes, nodes), f32),
                pltpu.VMEM((all_modes, nodes), f32),
                pltpu.VMEM((all_modes, samples), jnp.bfloat16),
                pltpu.VMEM((all_modes, samples), jnp.bfloat16),
                pltpu.VMEM((nodes, samples), f32),
                pltpu.VMEM((GEN_ROWS, samples), jnp.int32),
                pltpu.VMEM((modes, nodes), f32),
                pltpu.VMEM((width, 1, share), f32),
                pltpu.VMEM((width, 1, share), f32),
                pltpu.VMEM((1, share), f32),
                pltpu.VMEM((Z, 1, share), f32),
                pltpu.VMEM((1, share), f32),
                pltpu.SemaphoreType.DMA((3,)),
                pltpu.SemaphoreType.DMA((own,)),
                pltpu.SemaphoreType.DMA((own,)),
                pltpu.SemaphoreType.DMA((own,)),
                pltpu.SemaphoreType.DMA((2 * X * Z,)),
                pltpu.SemaphoreType.DMA((X * Z,)),
                pltpu.SemaphoreType.DMA((2 * width + Z,)),
                pltpu.SemaphoreType.DMA((2 * width + Z,)),
                pltpu.SemaphoreType.DMA,
            ],
            compiler_params=pltpu.CompilerParams(
                collective_id=0, has_side_effects=True, vmem_limit_bytes=60 * 1024 * 1024
            ),
        )(mode_basis, mode_scales[None, :], mean_log[None, :], sample_seeds[None, :])
        parts = 4
        shapes = (jax.ShapeDtypeStruct(modulus.shape, f32), jax.ShapeDtypeStruct(means.shape, f32))
        modulus, means = pl.pallas_call(
            hand_over,
            out_shape=shapes,
            in_specs=[pl.BlockSpec(memory_space=pl.ANY)] * 2,
            out_specs=(pl.BlockSpec(memory_space=pl.ANY),) * 2,
            scratch_shapes=[
                pltpu.VMEM(modulus.shape, f32),
                pltpu.VMEM(means.shape, f32),
                pltpu.SemaphoreType.DMA((parts + 1,)),
                pltpu.SemaphoreType.DMA((parts + 1,)),
            ],
            compiler_params=pltpu.CompilerParams(vmem_limit_bytes=60 * 1024 * 1024),
        )(modulus, means)
        return modulus, means.reshape(samples)

    return jax.shard_map(
        on_device,
        mesh=mesh,
        in_specs=(P("mode", "node"), P("mode"), P(("node", "mode")), P("grp")),
        out_specs=(P(("node", "mode"), "grp"), P("grp")),
        check_vma=False,
    )
```

```python
import functools
import math

import jax
import jax.numpy as jnp
from jax import lax
from jax.experimental import pallas as pl
from jax.experimental.pallas import tpu as pltpu
from jax.sharding import PartitionSpec as P

MESH = pl.DeviceIdType.MESH
X, Z = 4, 16
C1, C2 = -1640531527, 668265261
H1, H2 = -2048144789, -1028477387
OFFSETS = (4, -4, 3, -3, 8, 7, -7, 6, -6, 5, -5, 2, -2, 1, -1, 0)
NEAR = 4
NEAR_FIRST = 4
SPLIT = 13
AHEAD = 3
LEAD = 9
GEN_ROWS, GEN_COLS = 16, 512


def pieces_sent(groups):
    if groups > X:
        return X * Z // groups
    return SPLIT * (X // groups) + (Z - SPLIT) * X


def wrap32(value):
    return ((value + 2**31) % 2**32) - 2**31


SINE_TURNS = (6.283185160089197, -41.3416550313564, 81.60100406980851, -76.54978221989163, 39.536705541154184)
SINE = [c * math.sqrt(2.0) for c in SINE_TURNS]


def mix(word):
    word = word ^ lax.shift_right_logical(word, 15)
    word = word * H1
    word = word ^ lax.shift_right_logical(word, 13)
    word = word * H2
    return word ^ lax.shift_right_logical(word, 16)


def normals_tile(seed_part, mode_part):
    start = seed_part + mode_part
    first = mix(start)
    second = mix(start + C2)
    unit = ((first & 16777215).astype(jnp.float32) + 0.5) * (1.0 / 16777216.0)
    minus_log = jnp.maximum(-jnp.log(unit), 1e-30)
    radius = minus_log * lax.rsqrt(minus_log)
    turn = (lax.shift_left(second, 8) | 128).astype(jnp.float32)
    w = 0.25 - jnp.abs(turn * (1.0 / 4294967296.0))
    s = w * w
    p = SINE[4]
    for c in (SINE[3], SINE[2], SINE[1], SINE[0]):
        p = p * s + c
    return radius * (p * w)


def kernel(
    groups, basis, scales, mean_log, seeds, out_hbm, means_out,
    small_s, small_m, small_d, send_buf, recv, chi, clo, acc, seed_rows, mode_col, part, row_buf, row_sum, col_buf, fin,
    in_sem, load_sem, tx_sem, rx_sem, ytx_sem, yrx_sem, red_tx, red_rx, out_sem, far_sem,
):
    own = pieces_sent(groups)
    rows = basis.shape[0]
    chunk_rows = X * rows
    per = max(X // groups, 1)
    right_hops, left_hops = groups // 2, (groups - 1) // 2
    samples = seeds.shape[1]
    cores = lax.axis_size("node")
    nodes = acc.shape[0]

    grp = lax.axis_index("grp")
    me = lax.axis_index("mode")
    core = lax.axis_index("node")
    x, z = me // Z, lax.rem(me, Z)

    def wrap(value, size):
        return jnp.where(value >= size, value - size, value)

    def z_offset(t):
        if isinstance(t, int):
            return OFFSETS[t] % Z
        value = jnp.int32(OFFSETS[-1] % Z)
        for place, offset in enumerate(OFFSETS[:-1]):
            value = jnp.where(t == place, offset % Z, value)
        return value

    def number(plane, i):
        return i * groups + plane

    def ahead(dx, dz):
        return wrap(x + dx, X) * Z + wrap(z + dz, Z)

    def behind(dx, dz):
        return wrap(x - dx + X, X) * Z + wrap(z - dz + Z, Z)

    self_number = OFFSETS.index(0) * X

    def pieces_at(t):
        if t < SPLIT:
            return [(t * per + r, r * groups + grp) for r in range(per)]
        return [(SPLIT * per + (t - SPLIT) * X + dx, dx) for dx in range(X)]

    if groups <= X:
        pieces = [(i, t, dx) for t in range(len(OFFSETS)) for i, dx in pieces_at(t)]
        self_piece = SPLIT * per + (OFFSETS.index(0) - SPLIT) * X
    else:
        pieces = []
        for i in range(own):
            e = number(grp, i)
            pieces.append((i, lax.div(e, X), lax.rem(e, X)))
        self_piece = self_number // groups

    right = lax.rem(grp + 1, groups)
    left = lax.rem(grp + groups - 1, groups)

    bar = pltpu.get_barrier_semaphore()

    def hello(**where):
        pl.semaphore_signal(bar, 1, device_id=where, device_id_type=MESH)

    def row_peer(d):
        q = wrap(x * cores + core + d, X * cores)
        qx = lax.div(q, cores)
        return {"mode": qx * Z + z, "node": q - qx * cores}

    def load(i, t, dx):
        col = pl.multiple_of(ahead(dx, z_offset(t)) * nodes, nodes)
        return pltpu.make_async_copy(basis.at[:, pl.ds(col, nodes)], send_buf.at[i], load_sem.at[i])

    for args in pieces[: AHEAD + 1]:
        load(*args).start()

    columns = [r * groups + grp for r in range(per)] if groups <= X else range(X)

    @pl.loop(0, 2 * NEAR + 1)
    def _(k):
        dz = wrap(k + Z - NEAR, Z)
        for dx in columns:

            @pl.when(jnp.logical_or(dz != 0, dx != 0))
            def _():
                hello(mode=behind(dx, dz))

        @pl.when(dz != 0)
        def _():
            hello(mode=behind(0, dz))

    beside = [(dx, dz) for dz in (1, Z - 1) for dx in range(1, X)] if groups <= X else []
    for dx, dz in beside:
        hello(mode=behind(dx, dz))

    small = [
        pltpu.make_async_copy(source, target, in_sem.at[k])
        for k, (source, target) in enumerate(((scales, small_s), (mean_log, small_m), (seeds, small_d)))
    ]
    for copy in small:
        copy.start()

    for args in pieces[AHEAD + 1 :]:
        load(*args).start()

    @pl.loop(1, X * cores)
    def _(d):
        hello(**row_peer(d))

    if right_hops:
        hello(grp=left)
    if left_hops:
        hello(grp=right)

    for copy in small:
        copy.wait()
    row64 = lax.broadcasted_iota(jnp.int32, (64, 64), 0)
    col64 = lax.broadcasted_iota(jnp.int32, (64, 64), 1)
    scale_col = jnp.sum(
        jnp.where(row64 == col64, jnp.broadcast_to(small_s[...], (64, 64)), 0.0), axis=1, keepdims=True
    )
    mode_col[...] = jnp.broadcast_to(scale_col, mode_col.shape)

    def scale(i):
        load(i, 0, 0).wait()
        send_buf[i] = send_buf[i] * mode_col[...]

    for i in range(min(AHEAD, own)):
        scale(i)

    own_columns = len(columns) if groups <= X else X
    no_self = jnp.where(grp == 0, 1, 0) if groups <= X else 1
    expected = (2 * NEAR + 1) * own_columns - no_self + 2 * NEAR + len(beside) + (X * cores - 1)
    expected = expected + (1 if right_hops else 0) + (1 if left_hops else 0)
    pl.semaphore_wait(bar, expected)

    for side, dz in enumerate((Z - NEAR, NEAR)):
        pl.semaphore_signal(far_sem.at[side], 1, device_id={"mode": ahead(0, dz)}, device_id_type=MESH)

    def slot(e):
        return recv.at[pl.ds(pl.multiple_of(e * rows, rows), rows), :]

    def piece(i, t, dx):
        return pltpu.make_async_remote_copy(
            src_ref=send_buf.at[i],
            dst_ref=slot(t * X + dx),
            send_sem=tx_sem.at[i],
            recv_sem=rx_sem.at[i],
            device_id={"mode": ahead(dx, z_offset(t))},
            device_id_type=MESH,
        )

    def send_piece(i, t, dx):
        @pl.when(t * X + dx != self_number)
        def _():
            piece(i, t, dx).start()

    first_far = NEAR_FIRST * per if groups <= X else 0
    for i, t, dx in pieces:
        if i == first_far:
            for side in (0, 1):
                pl.semaphore_wait(far_sem.at[side], 1)
        if i + AHEAD < own:
            scale(i + AHEAD)
        send_piece(i, t, dx)

    has_self = True if groups <= X else grp == self_number % groups

    @pl.when(has_self)
    def _():
        recv[self_number * rows : (self_number + 1) * rows, :] = send_buf[self_piece]

    def hop(e, direction):
        return pltpu.make_async_remote_copy(
            src_ref=slot(e),
            dst_ref=slot(e),
            send_sem=ytx_sem.at[direction * X * Z + e],
            recv_sem=yrx_sem.at[e],
            device_id={"grp": (right, left)[direction]},
            device_id_type=MESH,
        )

    row_n = lax.broadcasted_iota(jnp.int32, (nodes, nodes), 0)
    col_n = lax.broadcasted_iota(jnp.int32, (nodes, nodes), 1)
    mean_col = jnp.sum(
        jnp.where(row_n == col_n, jnp.broadcast_to(small_m[...], (nodes, nodes)), 0.0), axis=1, keepdims=True
    )
    acc[...] = jnp.broadcast_to(mean_col, acc.shape)
    seed_rows[...] = jnp.broadcast_to(small_d[...] * C1, seed_rows.shape)

    row_ids = lax.broadcasted_iota(jnp.int32, (GEN_ROWS, GEN_COLS), 0) * wrap32(2 * C2)

    def generate(chunk):
        @pl.loop(0, X)
        def _(dx):
            first_mode = behind(dx, z_offset(chunk)) * rows
            first_row = (chunk * X + dx) * rows

            @pl.loop(0, rows // GEN_ROWS)
            def _(r):
                mode_part = row_ids + (first_mode + r * GEN_ROWS) * wrap32(2 * C2)
                at = pl.ds(pl.multiple_of(first_row + r * GEN_ROWS, GEN_ROWS), GEN_ROWS)
                for c in range(samples // GEN_COLS):
                    cols = slice(c * GEN_COLS, (c + 1) * GEN_COLS)
                    value = normals_tile(seed_rows[:, cols], mode_part)
                    high = value.astype(jnp.bfloat16)
                    chi[at, cols] = high
                    clo[at, cols] = (value - high.astype(jnp.float32)).astype(jnp.bfloat16)

    def contract(chunk):
        at = pl.ds(pl.multiple_of(chunk * chunk_rows, chunk_rows), chunk_rows)
        lhs = recv[at, :].T
        high = lhs.astype(jnp.bfloat16)
        low = (lhs - high.astype(jnp.float32)).astype(jnp.bfloat16)
        dot = functools.partial(jnp.dot, preferred_element_type=jnp.float32)
        for c in range(samples // 256):
            cols = slice(c * 256, (c + 1) * 256)
            c_high = chi[at, cols]
            acc[:, cols] += dot(high, c_high) + dot(low, c_high) + dot(high, clo[at, cols])

    def arrive(i, t, dx, travels=True):
        @pl.when(t * X + dx != self_number)
        def _():
            piece(i, t, dx).wait_recv()

        if travels and right_hops:
            hop(t * X + dx, 0).start()
        if travels and left_hops:
            hop(t * X + dx, 1).start()

    def ring_plane(b):
        hops = (b + 1) // 2
        return lax.rem(grp + (groups - hops if b % 2 else hops), groups)

    def goes_on(b):
        return (b + 1) // 2 < (right_hops if b % 2 else left_hops)

    chunks = len(OFFSETS)
    if groups <= X:

        @pl.loop(0, LEAD)
        def _(t):
            generate(t)

        @pl.loop(0, SPLIT + 1)
        def _(t):
            @pl.when(t < SPLIT)
            def _():
                for r in range(per):
                    arrive(t * per + r, t, r * groups + grp)

            @pl.when(t > 0)
            def _():
                for b in range(1, groups):
                    for r in range(per):
                        e = (t - 1) * X + r * groups + ring_plane(b)
                        hop(e, 0).wait_recv()
                        if goes_on(b):
                            hop(e, (b + 1) % 2).start()
                contract(t - 1)

            @pl.when(t + LEAD < chunks)
            def _():
                generate(t + LEAD)

        @pl.loop(SPLIT, chunks)
        def _(t):
            for dx in range(X):
                arrive(SPLIT * per + (t - SPLIT) * X + dx, t, dx, travels=False)
            contract(t)

    else:
        step = chunks // groups

        def generate_some(b):
            @pl.loop(0, step)
            def _(k):
                generate(b * step + k)

        generate_some(0)

        @pl.loop(0, own)
        def _(i):
            e = number(grp, i)
            t = lax.div(e, X)
            arrive(i, t, e - t * X)

        for b in range(1, groups):
            generate_some(b)

            @pl.loop(0, own)
            def _(i, b=b):
                e = number(ring_plane(b), i)
                hop(e, 0).wait_recv()
                if goes_on(b):
                    hop(e, (b + 1) % 2).start()

        @pl.loop(0, chunks)
        def _(t):
            contract(t)

    def all_sent():
        @pl.loop(0, own)
        def _(i):
            @pl.when(jnp.logical_not(jnp.logical_and(has_self, i == self_piece)))
            def _():
                piece(i, 0, 0).wait_send()

        @pl.loop(0, SPLIT * per if groups <= X else own)
        def _(i):
            e = number(grp, i)
            for direction, hops in enumerate((right_hops, left_hops)):
                if hops:
                    hop(e, direction).wait_send()
            for b in range(1, groups):
                if goes_on(b):
                    hop(number(ring_plane(b), i), (b + 1) % 2).wait_send()

    for c in range(samples // 256):
        cols = slice(c * 256, (c + 1) * 256)
        value = jnp.exp(acc[:, cols])
        acc[:, cols] = value
        part[c] = jnp.sum(value, axis=0, keepdims=True)
    store = pltpu.make_async_copy(acc, out_hbm, out_sem)
    store.start()

    me_row = x * cores + core
    width = X * cores

    def row_copy(source, target, d, slot):
        return pltpu.make_async_remote_copy(
            src_ref=source, dst_ref=target, send_sem=red_tx.at[slot], recv_sem=red_rx.at[slot],
            device_id=row_peer(d), device_id_type=MESH,
        )

    @pl.loop(1, width)
    def _(d):
        row_copy(part.at[wrap(me_row + d, width)], row_buf.at[me_row], d, d).start()

    row_buf[me_row] = part[me_row]

    @pl.loop(1, width)
    def _(d):
        row_copy(part.at[me_row], row_buf.at[me_row], d, d).wait()

    total = row_buf[0]
    for k in range(1, width):
        total = total + row_buf[k]
    row_sum[...] = total

    def column_copy(k):
        return pltpu.make_async_remote_copy(
            src_ref=row_sum, dst_ref=col_buf.at[z], send_sem=red_tx.at[width + k], recv_sem=red_rx.at[width + k],
            device_id={"mode": ahead(0, k)}, device_id_type=MESH,
        )

    for k in sorted(range(1, Z), key=lambda k: -min(k, Z - k)):
        column_copy(k).start()

    col_buf[z] = total

    @pl.loop(1, Z)
    def _(k):
        column_copy(k).wait()

    total = col_buf[0]
    for k in range(1, Z):
        total = total + col_buf[k]
    node_count = nodes * X * Z * cores
    fin[...] = total * (1.0 / node_count)

    @pl.loop(1, width)
    def _(d):
        row_copy(fin, means_out.at[me_row], d, width + Z + d).start()

    means_out[me_row] = fin[...]

    @pl.loop(1, width)
    def _(d):
        row_copy(fin, means_out.at[me_row], d, width + Z + d).wait()

    all_sent()
    store.wait()


def hand_over(modulus, means, modulus_out, means_out, held, held_means, in_sem, out_sem):
    parts = in_sem.shape[0] - 1
    rows = modulus.shape[0] // parts
    spans = [pl.ds(k * rows, rows) for k in range(parts)]
    steps = [(modulus.at[at], held.at[at], modulus_out.at[at]) for at in spans] + [(means, held_means, means_out)]
    copies_in = [pltpu.make_async_copy(a, b, in_sem.at[k]) for k, (a, b, _) in enumerate(steps)]
    copies_out = [pltpu.make_async_copy(b, c, out_sem.at[k]) for k, (_, b, c) in enumerate(steps)]
    for copy in copies_in:
        copy.start()
    for arrived, onward in zip(copies_in, copies_out):
        arrived.wait()
        onward.start()
    for copy in copies_out:
        copy.wait()


def solution(mesh):
    groups = mesh.shape["grp"]

    def on_device(mode_basis, mode_scales, mean_log, sample_seeds):
        modes = mode_basis.shape[0]
        nodes, samples = mean_log.shape[0], sample_seeds.shape[0]
        all_modes = modes * X * Z
        own = pieces_sent(groups)
        width = X * mesh.shape["node"]
        share = samples // width
        f32 = jnp.float32
        vmem = pl.BlockSpec(memory_space=pltpu.VMEM)
        modulus, means = pl.pallas_call(
            functools.partial(kernel, groups),
            out_shape=(jax.ShapeDtypeStruct((nodes, samples), f32), jax.ShapeDtypeStruct((width, 1, share), f32)),
            in_specs=[pl.BlockSpec(memory_space=pl.ANY)] * 4,
            out_specs=(pl.BlockSpec(memory_space=pl.ANY), vmem),
            scratch_shapes=[
                pltpu.VMEM((1, modes), f32),
                pltpu.VMEM((1, nodes), f32),
                pltpu.VMEM((1, samples), jnp.int32),
                pltpu.VMEM((own, modes, nodes), f32),
                pltpu.VMEM((all_modes, nodes), f32),
                pltpu.VMEM((all_modes, samples), jnp.bfloat16),
                pltpu.VMEM((all_modes, samples), jnp.bfloat16),
                pltpu.VMEM((nodes, samples), f32),
                pltpu.VMEM((GEN_ROWS, samples), jnp.int32),
                pltpu.VMEM((modes, nodes), f32),
                pltpu.VMEM((width, 1, share), f32),
                pltpu.VMEM((width, 1, share), f32),
                pltpu.VMEM((1, share), f32),
                pltpu.VMEM((Z, 1, share), f32),
                pltpu.VMEM((1, share), f32),
                pltpu.SemaphoreType.DMA((3,)),
                pltpu.SemaphoreType.DMA((own,)),
                pltpu.SemaphoreType.DMA((own,)),
                pltpu.SemaphoreType.DMA((own,)),
                pltpu.SemaphoreType.DMA((2 * X * Z,)),
                pltpu.SemaphoreType.DMA((X * Z,)),
                pltpu.SemaphoreType.DMA((2 * width + Z,)),
                pltpu.SemaphoreType.DMA((2 * width + Z,)),
                pltpu.SemaphoreType.DMA,
                pltpu.SemaphoreType.REGULAR((2,)),
            ],
            compiler_params=pltpu.CompilerParams(
                collective_id=0, has_side_effects=True, vmem_limit_bytes=60 * 1024 * 1024
            ),
        )(mode_basis, mode_scales[None, :], mean_log[None, :], sample_seeds[None, :])
        parts = 4
        shapes = (jax.ShapeDtypeStruct(modulus.shape, f32), jax.ShapeDtypeStruct(means.shape, f32))
        modulus, means = pl.pallas_call(
            hand_over,
            out_shape=shapes,
            in_specs=[pl.BlockSpec(memory_space=pl.ANY)] * 2,
            out_specs=(pl.BlockSpec(memory_space=pl.ANY),) * 2,
            scratch_shapes=[
                pltpu.VMEM(modulus.shape, f32),
                pltpu.VMEM(means.shape, f32),
                pltpu.SemaphoreType.DMA((parts + 1,)),
                pltpu.SemaphoreType.DMA((parts + 1,)),
            ],
            compiler_params=pltpu.CompilerParams(vmem_limit_bytes=60 * 1024 * 1024),
        )(modulus, means)
        return modulus, means.reshape(samples)

    return jax.shard_map(
        on_device,
        mesh=mesh,
        in_specs=(P("mode", "node"), P("mode"), P(("node", "mode")), P("grp")),
        out_specs=(P(("node", "mode"), "grp"), P("grp")),
        check_vma=False,
    )
```
